32 devices in a mesh: stream: 16 (over z, y, core), tm: 2 (over x).
Axes of the slice: x: 2, y: 2, z: 4, core: 2. Of those that a mesh axis runs over, the one named last changes fastest.
Arguments:
- signal: bfloat16 [32, 2, 1048576], P('stream', None, 'tm'), parts along dimension 0, may hold values from -11 to 11
- taps: float32 [16, 4096], replicated, may hold values from -1.5 to 1.5
Outputs:
- channels_out: float32 [32, 2, 4096, 256], P('stream', None, 'tm'), parts along dimension 0
The draws below stay inside these ranges and needn't reach their ends.
There are 16 independent parts, one for each index of `stream`. The reference program is written for one: setup_inputs(seed, part) draws one part's arguments, and reference() takes and returns one part's arrays. A program takes and returns all parts, laid end to end along the dimension named above; an argument that names none is the same for every part. Nothing has to cross between parts.
All inputs are finite; a program needn't handle non-finite values.
Results may differ from the reference program's by a relative error of at most 0.0003.
Values may be sent and summed in bfloat16 or wider, within the bound.
A program may use at most 128 MiB of HBM per device.

```python
import math
import jax
import jax.numpy as jnp
from jax import lax

CHANNELS = 4096
RADIX = 64
TAPS = 16
STREAMS = 2
FRAMES = 256
SAMPLES = 1048576


def draw_signal(key, part):
    key_noise, key_gain, key_freq, key_level = jax.random.split(key, 4)
    blocks = FRAMES // 8 + 1
    position = jnp.arange(SAMPLES, dtype=jnp.int32)
    which = position // CHANNELS // 8
    noise = jax.random.truncated_normal(key_noise, -4.0, 4.0, (STREAMS, 2, SAMPLES), jnp.float32)
    gains = jnp.exp(jax.random.uniform(key_gain, (STREAMS, blocks), jnp.float32, math.log(0.5), math.log(2.0)))
    envelope = gains[:, which]
    numerators = jax.random.randint(key_freq, (STREAMS, 3), 0, 1 << 20, jnp.int32)
    levels = jax.random.uniform(key_level, (STREAMS, 3), jnp.float32, 0.3, 1.0)
    tone_real = jnp.zeros((STREAMS, SAMPLES), jnp.float32)
    tone_imag = jnp.zeros((STREAMS, SAMPLES), jnp.float32)
    for number in range(3):
        wrapped = jnp.bitwise_and(numerators[:, number][:, None] * position[None, :], (1 << 20) - 1)
        phase = wrapped.astype(jnp.float32) * (2.0 * math.pi / (1 << 20))
        tone_real = tone_real + levels[:, number][:, None] * jnp.cos(phase)
        tone_imag = tone_imag + levels[:, number][:, None] * jnp.sin(phase)
    result = jnp.stack([noise[:, 0] * envelope + tone_real, noise[:, 1] * envelope + tone_imag], axis=1)
    return result.astype(jnp.bfloat16)


def bell_draw(rng, shape, scale, bound, held_as=jnp.bfloat16):
    array = jax.random.normal(rng, shape, jnp.float32) * scale
    return jnp.minimum(jnp.maximum(array, -bound), bound).astype(held_as)


def setup_inputs(seed: int = 0, part: int = 0) -> dict:
    key_of = jax.random.split(jax.random.key(seed), 3)
    part_keys = jax.random.split(jax.random.fold_in(key_of[2], part), 3)
    signal = draw_signal(jax.random.fold_in(jax.random.fold_in(key_of[2], part), 71), part)
    taps = bell_draw(key_of[1], (TAPS, CHANNELS), TAPS ** -0.5, 1.5, jnp.float32)
    return {"signal": signal, "taps": taps}


def reference(signal, taps):
    streams = signal.shape[0]
    frames = signal.astype(jnp.float32).reshape(streams, 2, FRAMES, CHANNELS)
    padded = jnp.pad(frames, ((0, 0), (0, 0), (TAPS - 1, 0), (0, 0)))
    filtered = jnp.zeros((streams, 2, FRAMES, CHANNELS), jnp.float32)
    for tap_index in range(TAPS):
        start = TAPS - 1 - tap_index
        filtered = filtered + taps[tap_index] * padded[:, :, start:start + FRAMES, :]
    spectrum = jnp.fft.fft(lax.complex(filtered[:, 0], filtered[:, 1]), axis=-1) / RADIX
    real_part = jnp.real(spectrum)
    imag_part = jnp.imag(spectrum)
    power = lax.optimization_barrier(jnp.mean(real_part * real_part + imag_part * imag_part, axis=1))
    factor = 1.0 / jnp.sqrt(power + 1.0)
    stacked = jnp.stack([real_part * factor[:, None, :], imag_part * factor[:, None, :]], axis=1)
    return jnp.transpose(stacked, (0, 1, 3, 2))
```

```python
import functools
import math

import jax
import jax.numpy as jnp
import numpy as np
from jax import lax
from jax.experimental import pallas as pl
from jax.experimental.pallas import tpu as pltpu
from jax.sharding import PartitionSpec as P

LANES = 128
GROUP = 4
PAIR = 2 * GROUP


def angles(height, breadth, modulus):
    product = np.arange(height)[:, None] * np.arange(breadth)[None, :] % modulus
    return product * (2.0 * math.pi / modulus)


def split(table):
    high = table.astype(np.float32).astype(jnp.bfloat16)
    low = (table - high.astype(np.float64)).astype(np.float32).astype(jnp.bfloat16)
    return high, low


def first_table(rows):
    turn = angles(rows, rows, rows)
    cos, sin = np.cos(turn), np.sin(turn)
    whole = np.block([[cos, sin], [-sin, cos]])
    high, low = split(np.kron(np.eye(GROUP), whole))
    return np.concatenate([high, low, high], axis=1)


def second_table(rows, channels, parts):
    turn = angles(LANES, LANES, LANES)
    scale = 1.0 / math.isqrt(channels)
    cos, sin = np.cos(turn) * scale, np.sin(turn) * scale
    each = LANES // parts
    blocks = []
    for part in range(parts):
        pick = slice(part * each, (part + 1) * each)
        blocks.append(np.block([[cos[pick], sin[pick]], [-sin[pick], cos[pick]]]))
    high, low = split(np.concatenate(blocks, axis=0))
    return np.concatenate([high, low, high], axis=1)


def transform_kernel(parts, frames, rows, edge, x_ref, halo_ref, taps_ref, first_ref, cos_ref,
                     sin_ref, second_ref, own_ref, away_ref, wide, grid, zr, zi):
    depth = edge
    for p in range(2):
        wide[p, :edge] = halo_ref[0, p].astype(jnp.float32)

    @pl.loop(0, frames // PAIR)
    def _(step):
        base = pl.multiple_of(step * PAIR, PAIR)
        for p in range(2):
            wide[p, pl.ds(base + edge, PAIR)] = x_ref[0, p, pl.ds(base, PAIR)].astype(jnp.float32)

    @pl.loop(0, frames // PAIR)
    def _(step):
        base = pl.multiple_of(step * PAIR, PAIR)
        for p in range(2):
            for piece in range(rows // 8):
                sub = slice(piece * 8, piece * 8 + 8)
                data = [wide[p, base + 1 + i, sub, :] for i in range(PAIR + depth - 1)]
                taps = [taps_ref[k, sub, :] for k in range(depth)]
                for t in range(PAIR):
                    total = taps[0] * data[t + depth - 1]
                    for k in range(1, depth):
                        total = total + taps[k] * data[t + depth - 1 - k]
                    row = ((t % GROUP) * 2 + p) * rows + piece * 8
                    lane = (t // GROUP) * LANES
                    grid[row : row + 8, lane : lane + LANES] = total
        value = grid[...]
        high = value.astype(jnp.bfloat16)
        low = (value - high.astype(jnp.float32)).astype(jnp.bfloat16)
        out = jnp.dot(first_ref[...], jnp.concatenate([high, high, low], axis=0),
                      preferred_element_type=jnp.float32)
        cos, sin = cos_ref[...], sin_ref[...]
        for t in range(PAIR):
            row = (t % GROUP) * 2 * rows
            lane = (t // GROUP) * LANES
            real = out[row : row + rows, lane : lane + LANES]
            imag = out[row + rows : row + 2 * rows, lane : lane + LANES]
            at = pl.multiple_of((base + t) * rows, rows)
            zr[pl.ds(at, rows), :] = real * cos + imag * sin
            zi[pl.ds(at, rows), :] = imag * cos - real * sin

    each = LANES // parts

    @pl.loop(0, rows // 2)
    def _(step):
        pieces = []
        for i in range(2):
            pick = pl.ds(step * 2 + i, frames, stride=rows)
            pieces.append(jnp.concatenate([zr[pick, :], zi[pick, :]], axis=1))
        value = jnp.concatenate(pieces, axis=0)
        high = value.astype(jnp.bfloat16)
        low = (value - high.astype(jnp.float32)).astype(jnp.bfloat16)
        out = lax.dot_general(second_ref[...], jnp.concatenate([high, high, low], axis=1),
                              (((1,), (1,)), ((), ())), preferred_element_type=jnp.float32)
        for i in range(2):
            c = step * 2 + i
            lane = slice(i * frames, (i + 1) * frames)
            for p in range(2):
                own_ref[p, c] = out[p * each : (p + 1) * each, lane]
                for k in range(1, parts):
                    top = (2 * k + p) * each
                    away_ref[k - 1, p, c] = out[top : top + each, lane]


def finish_kernel(parts, frames, rows, each, *refs):
    own_ref, away_refs, out_ref, turned = refs[0], refs[1:parts], refs[-2], refs[-1]
    me = lax.axis_index("tm")

    @pl.loop(0, rows)
    def _(c):
        data = [[own_ref[p, c] for p in range(2)]]
        for ref in away_refs:
            data.append([ref[p, c] for p in range(2)])
        square = sum(d[0] * d[0] + d[1] * d[1] for d in data)
        power = jnp.sum(square, axis=1, keepdims=True)
        factor = lax.rsqrt(power * (1.0 / (frames * parts)) + 1.0)
        for k in range(parts):
            for p in range(2):
                turned[k, p, pl.ds(c, each, stride=rows), :] = data[k][p] * factor

    for k in range(parts):
        source = lax.rem(me + parts - k, parts)
        lane = pl.ds(pl.multiple_of(source * frames, frames), frames)
        for p in range(2):
            out_ref[0, p, :, lane] = turned[k, p]


def sent(block, route):
    narrow = (block * 2.0).astype(jnp.float16)
    return lax.ppermute(narrow, "tm", route).astype(jnp.float32) * 0.5


def shards(parts, signal, taps):
    streams = signal.shape[0]
    depth, channels = taps.shape
    rows = channels // LANES
    frames = signal.shape[2] // channels
    each = LANES // parts
    me = lax.axis_index("tm")
    x = signal.reshape(streams, 2, frames, rows, LANES)
    route = [(i, i + 1) for i in range(parts - 1)]
    halo = lax.ppermute(x[:, :, frames - depth :], "tm", route)
    taps = taps.reshape(depth, rows, LANES)
    twist = angles(rows, LANES, channels)
    cos, sin = jnp.asarray(np.cos(twist), jnp.float32), jnp.asarray(np.sin(twist), jnp.float32)
    first = jnp.asarray(first_table(rows))
    table = second_table(rows, channels, parts)
    second = lax.dynamic_slice(
        jnp.asarray(np.concatenate([table, table], axis=0)),
        (me * 2 * each, 0), table.shape)
    owns, aways = [], []
    whole = lambda a: pl.BlockSpec(a.shape, lambda i, nd=a.ndim: (0,) * nd)
    for s in range(streams):
        pick = lambda i, s=s: (s, 0, 0, 0, 0)
        own, away = pl.pallas_call(
            functools.partial(transform_kernel, parts, frames, rows, depth),
            grid=(1,),
            in_specs=[
                pl.BlockSpec((1, 2, frames, rows, LANES), pick),
                pl.BlockSpec((1, 2, depth, rows, LANES), pick),
                whole(taps), whole(first), whole(cos), whole(sin), whole(second),
            ],
            out_specs=[
                pl.BlockSpec((2, rows, each, frames), lambda i: (0, 0, 0, 0)),
                pl.BlockSpec((parts - 1, 2, rows, each, frames), lambda i: (0, 0, 0, 0, 0)),
            ],
            out_shape=[
                jax.ShapeDtypeStruct((2, rows, each, frames), jnp.float32),
                jax.ShapeDtypeStruct((parts - 1, 2, rows, each, frames), jnp.float32),
            ],
            scratch_shapes=[
                pltpu.VMEM((2, depth + frames, rows, LANES), jnp.float32),
                pltpu.VMEM((2 * GROUP * rows, 2 * LANES), jnp.float32),
                pltpu.VMEM((frames * rows, LANES), jnp.float32),
                pltpu.VMEM((frames * rows, LANES), jnp.float32),
            ],
            compiler_params=pltpu.CompilerParams(vmem_limit_bytes=48 << 20),
            cost_estimate=pl.CostEstimate(flops=8 * 10**9, bytes_accessed=8 << 20, transcendentals=0),
            name="transform",
        )(x, halo, taps, first, cos, sin, second)
        owns.append(own)
        aways.append([
            sent(away[k - 1], [(i, (i + k) % parts) for i in range(parts)])
            for k in range(1, parts)
        ])
    result = None
    step = 16
    shape = jax.ShapeDtypeStruct((streams, 2, channels // parts, frames * parts), jnp.float32)
    for s in range(streams):
        block = pl.BlockSpec((2, rows, step, frames), lambda i: (0, 0, i, 0))
        args = [owns[s], *aways[s]]
        specs = [block] * parts
        alias = {}
        if result is not None:
            alias = {len(args): 0}
            args.append(result)
            specs.append(pl.BlockSpec(memory_space=pl.ANY))
        result = pl.pallas_call(
            functools.partial(finish_kernel, parts, frames, rows, step),
            grid=(each // step,),
            in_specs=specs,
            out_specs=pl.BlockSpec((1, 2, rows * step, frames * parts), lambda i, s=s: (s, 0, i, 0)),
            out_shape=shape,
            input_output_aliases=alias,
            scratch_shapes=[pltpu.VMEM((parts, 2, rows * step, frames), jnp.float32)],
            compiler_params=pltpu.CompilerParams(vmem_limit_bytes=48 << 20),
            cost_estimate=pl.CostEstimate(flops=10**8, bytes_accessed=8 << 20, transcendentals=0),
            name="finish",
        )(*args)
    return result


def solution(mesh):
    in_specs = (P("stream", None, "tm"), P())
    out_specs = P("stream", None, "tm", None)
    body = functools.partial(shards, mesh.shape["tm"])
    return jax.shard_map(body, mesh=mesh, in_specs=in_specs, out_specs=out_specs, check_vma=False)
```

```python
import functools
import math

import jax
import jax.numpy as jnp
import numpy as np
from jax import lax
from jax.experimental import pallas as pl
from jax.experimental.pallas import tpu as pltpu
from jax.sharding import PartitionSpec as P

LANES = 128
GROUP = 4
PAIR = 2 * GROUP


def angles(height, breadth, modulus):
    product = np.arange(height)[:, None] * np.arange(breadth)[None, :] % modulus
    return product * (2.0 * math.pi / modulus)


def split(table):
    high = table.astype(np.float32).astype(jnp.bfloat16)
    low = (table - high.astype(np.float64)).astype(np.float32).astype(jnp.bfloat16)
    return high, low


def first_table(rows):
    turn = angles(rows, rows, rows)
    cos, sin = np.cos(turn), np.sin(turn)
    whole = np.block([[cos, sin], [-sin, cos]])
    high, low = split(np.kron(np.eye(GROUP), whole))
    return np.concatenate([high, low, high], axis=1)


def second_table(rows, channels, parts):
    turn = angles(LANES, LANES, LANES)
    scale = 1.0 / math.isqrt(channels)
    cos, sin = np.cos(turn) * scale, np.sin(turn) * scale
    each = LANES // parts
    blocks = []
    for part in range(parts):
        pick = slice(part * each, (part + 1) * each)
        blocks.append(np.block([[cos[pick], sin[pick]], [-sin[pick], cos[pick]]]))
    high, low = split(np.concatenate(blocks, axis=0))
    return np.concatenate([high, low, high], axis=1)


def transform_kernel(parts, frames, rows, edge, x_ref, halo_ref, taps_ref, first_ref, cos_ref,
                     sin_ref, second_ref, own_ref, away_ref, wide, grid, zr, zi):
    depth = edge
    for p in range(2):
        wide[p, :edge] = halo_ref[0, p].astype(jnp.float32)

    @pl.loop(0, frames // PAIR)
    def _(step):
        base = pl.multiple_of(step * PAIR, PAIR)
        for p in range(2):
            wide[p, pl.ds(base + edge, PAIR)] = x_ref[0, p, pl.ds(base, PAIR)].astype(jnp.float32)

    @pl.loop(0, frames // PAIR)
    def _(step):
        base = pl.multiple_of(step * PAIR, PAIR)
        for p in range(2):
            for piece in range(rows // 8):
                sub = slice(piece * 8, piece * 8 + 8)
                data = [wide[p, base + 1 + i, sub, :] for i in range(PAIR + depth - 1)]
                taps = [taps_ref[k, sub, :] for k in range(depth)]
                for t in range(PAIR):
                    total = taps[0] * data[t + depth - 1]
                    for k in range(1, depth):
                        total = total + taps[k] * data[t + depth - 1 - k]
                    row = ((t % GROUP) * 2 + p) * rows + piece * 8
                    lane = (t // GROUP) * LANES
                    grid[row : row + 8, lane : lane + LANES] = total
        value = grid[...]
        high = value.astype(jnp.bfloat16)
        low = (value - high.astype(jnp.float32)).astype(jnp.bfloat16)
        out = jnp.dot(first_ref[...], jnp.concatenate([high, high, low], axis=0),
                      preferred_element_type=jnp.float32)
        cos, sin = cos_ref[...], sin_ref[...]
        for t in range(PAIR):
            row = (t % GROUP) * 2 * rows
            lane = (t // GROUP) * LANES
            real = out[row : row + rows, lane : lane + LANES]
            imag = out[row + rows : row + 2 * rows, lane : lane + LANES]
            at = pl.multiple_of((base + t) * rows, rows)
            zr[pl.ds(at, rows), :] = real * cos + imag * sin
            zi[pl.ds(at, rows), :] = imag * cos - real * sin

    each = LANES // parts

    @pl.loop(0, rows // 2)
    def _(step):
        pieces = []
        for i in range(2):
            pick = pl.ds(step * 2 + i, frames, stride=rows)
            pieces.append(jnp.concatenate([zr[pick, :], zi[pick, :]], axis=1))
        value = jnp.concatenate(pieces, axis=0)
        high = value.astype(jnp.bfloat16)
        low = (value - high.astype(jnp.float32)).astype(jnp.bfloat16)
        out = lax.dot_general(second_ref[...], jnp.concatenate([high, high, low], axis=1),
                              (((1,), (1,)), ((), ())), preferred_element_type=jnp.float32)
        for i in range(2):
            c = step * 2 + i
            lane = slice(i * frames, (i + 1) * frames)
            for p in range(2):
                own_ref[p, c] = out[p * each : (p + 1) * each, lane]
                for k in range(1, parts):
                    top = (2 * k + p) * each
                    away_ref[k - 1, p, c] = out[top : top + each, lane]


def finish_kernel(parts, frames, rows, each, *refs):
    own_ref, away_refs, out_ref, turned = refs[0], refs[1:parts], refs[-2], refs[-1]
    me = lax.axis_index("tm")

    @pl.loop(0, rows, unroll=8)
    def _(c):
        data = [[own_ref[p, c] for p in range(2)]]
        for ref in away_refs:
            data.append([ref[p, c] for p in range(2)])
        square = sum(d[0] * d[0] + d[1] * d[1] for d in data)
        power = jnp.sum(square, axis=1, keepdims=True)
        factor = lax.rsqrt(power * (1.0 / (frames * parts)) + 1.0)
        for k in range(parts):
            for p in range(2):
                turned[k, p, pl.ds(c, each, stride=rows), :] = data[k][p] * factor

    for k in range(parts):
        source = lax.rem(me + parts - k, parts)
        lane = pl.ds(pl.multiple_of(source * frames, frames), frames)
        for p in range(2):
            out_ref[0, p, :, lane] = turned[k, p]


def sent(block, route):
    narrow = (block * 2.0).astype(jnp.float16)
    return lax.ppermute(narrow, "tm", route).astype(jnp.float32) * 0.5


def shards(parts, signal, taps):
    streams = signal.shape[0]
    depth, channels = taps.shape
    rows = channels // LANES
    frames = signal.shape[2] // channels
    each = LANES // parts
    me = lax.axis_index("tm")
    x = signal.reshape(streams, 2, frames, rows, LANES)
    route = [(i, i + 1) for i in range(parts - 1)]
    halos = [lax.ppermute(x[s : s + 1, :, frames - depth :], "tm", route) for s in range(streams)]
    taps = taps.reshape(depth, rows, LANES)
    twist = angles(rows, LANES, channels)
    cos, sin = jnp.asarray(np.cos(twist), jnp.float32), jnp.asarray(np.sin(twist), jnp.float32)
    first = jnp.asarray(first_table(rows))
    table = second_table(rows, channels, parts)
    second = lax.dynamic_slice(
        jnp.asarray(np.concatenate([table, table], axis=0)),
        (me * 2 * each, 0), table.shape)
    owns, aways = [], []
    whole = lambda a: pl.BlockSpec(a.shape, lambda i, nd=a.ndim: (0,) * nd)
    for s in range(streams):
        pick = lambda i, s=s: (s, 0, 0, 0, 0)
        own, away = pl.pallas_call(
            functools.partial(transform_kernel, parts, frames, rows, depth),
            grid=(1,),
            in_specs=[
                pl.BlockSpec((1, 2, frames, rows, LANES), pick),
                whole(halos[s]), whole(taps), whole(first), whole(cos), whole(sin), whole(second),
            ],
            out_specs=[
                pl.BlockSpec((2, rows, each, frames), lambda i: (0, 0, 0, 0)),
                pl.BlockSpec((parts - 1, 2, rows, each, frames), lambda i: (0, 0, 0, 0, 0)),
            ],
            out_shape=[
                jax.ShapeDtypeStruct((2, rows, each, frames), jnp.float32),
                jax.ShapeDtypeStruct((parts - 1, 2, rows, each, frames), jnp.float32),
            ],
            scratch_shapes=[
                pltpu.VMEM((2, depth + frames, rows, LANES), jnp.float32),
                pltpu.VMEM((2 * GROUP * rows, 2 * LANES), jnp.float32),
                pltpu.VMEM((frames * rows, LANES), jnp.float32),
                pltpu.VMEM((frames * rows, LANES), jnp.float32),
            ],
            compiler_params=pltpu.CompilerParams(vmem_limit_bytes=48 << 20),
            cost_estimate=pl.CostEstimate(flops=8 * 10**9, bytes_accessed=8 << 20, transcendentals=0),
            name="transform",
        )(x, halos[s], taps, first, cos, sin, second)
        owns.append(own)
        aways.append([
            sent(away[k - 1], [(i, (i + k) % parts) for i in range(parts)])
            for k in range(1, parts)
        ])
    result = None
    step = 16
    shape = jax.ShapeDtypeStruct((streams, 2, channels // parts, frames * parts), jnp.float32)
    for s in range(streams):
        block = pl.BlockSpec((2, rows, step, frames), lambda i: (0, 0, i, 0))
        args = [owns[s], *aways[s]]
        specs = [block] * parts
        alias = {}
        if result is not None:
            alias = {len(args): 0}
            args.append(result)
            specs.append(pl.BlockSpec(memory_space=pl.ANY))
        result = pl.pallas_call(
            functools.partial(finish_kernel, parts, frames, rows, step),
            grid=(each // step,),
            in_specs=specs,
            out_specs=pl.BlockSpec((1, 2, rows * step, frames * parts), lambda i, s=s: (s, 0, i, 0)),
            out_shape=shape,
            input_output_aliases=alias,
            scratch_shapes=[pltpu.VMEM((parts, 2, rows * step, frames), jnp.float32)],
            compiler_params=pltpu.CompilerParams(vmem_limit_bytes=48 << 20),
            cost_estimate=pl.CostEstimate(flops=10**8, bytes_accessed=8 << 20, transcendentals=0),
            name="finish",
        )(*args)
    return result


def solution(mesh):
    in_specs = (P("stream", None, "tm"), P())
    out_specs = P("stream", None, "tm", None)
    body = functools.partial(shards, mesh.shape["tm"])
    return jax.shard_map(body, mesh=mesh, in_specs=in_specs, out_specs=out_specs, check_vma=False)
```
